32 devices in a mesh: row: 8 (over z, core), col: 4 (over y, x).
Axes of the slice: x: 2, y: 2, z: 4, core: 2. Of those that a mesh axis runs over, the one named last changes fastest.
Arguments:
- tokens: bfloat16 [512, 4096], P(None, 'col'), may hold values from -6 to 6
- w_gate: bfloat16 [4096, 10240], P('col', 'row'), may hold values from -0.09375 to 0.09375
- w_up: bfloat16 [4096, 10240], P('col', 'row'), may hold values from -0.09375 to 0.09375
- w_down: bfloat16 [10240, 4096], P('row', 'col'), may hold values from -0.0625 to 0.0625
Outputs:
- result: bfloat16 [512, 4096], P('row', 'col')
The draws below stay inside these ranges and needn't reach their ends.
All inputs are finite; a program needn't handle non-finite values.
Results may differ from the reference program's by a relative error of at most 0.025.
Values may be sent and summed in bfloat16 or wider, within the bound.
A program may use at most 64 MiB of HBM per device.

```python
import jax
import jax.numpy as jnp
from jax import lax

D = 4096
FF = 10240
TOKENS = 512
N_COL = 4


def block_levels(stream_key, extent, cuts, low, largest):
    def one(dim, shards_of):
        heights = jax.random.uniform(jax.random.fold_in(jax.random.fold_in(stream_key, 6), dim), (shards_of,), jnp.float32, low / len(cuts), largest / len(cuts))
        return jnp.repeat(jnp.exp(heights), extent[dim] // shards_of).reshape((-1,) + (1,) * (len(extent) - dim - 1))

    factor_of = one(*cuts[0])
    for cut in cuts[1:]:
        factor_of = factor_of * one(*cut)
    return factor_of


def gaussian(rng, dims, scale, reach, split=(), kind=jnp.bfloat16):
    gain = block_levels(rng, dims, split, -0.22, 0.18) if split else 1.0
    array = jax.random.normal(rng, dims, jnp.float32) * scale * gain
    return jnp.minimum(jnp.maximum(array, -reach), reach).astype(kind)


def setup_inputs(seed: int = 0) -> dict:
    key_of = jax.random.split(jax.random.key(seed), 5)
    return {
        "tokens": gaussian(key_of[0], (TOKENS, D), 1.0, 6.0, ((1, 4),)),
        "w_gate": gaussian(key_of[1], (D, FF), D ** -0.5, 0.09375, ((0, 4), (1, 8))),
        "w_up": gaussian(key_of[2], (D, FF), D ** -0.5, 0.09375, ((0, 4), (1, 8))),
        "w_down": gaussian(key_of[3], (FF, D), FF ** -0.5, 0.0625, ((0, 8), (1, 4))),
    }


def reference(tokens, w_gate, w_up, w_down):
    block_width = tokens.shape[1] // N_COL
    joined = jnp.concatenate([w_gate, w_up], axis=1)
    hidden_width = w_gate.shape[1]

    def accumulate(running, block_index):
        offset = (block_index * block_width).astype(jnp.int32)
        token_rows = lax.dynamic_slice_in_dim(tokens, offset, block_width, 1)
        weight_rows = lax.dynamic_slice_in_dim(joined, offset, block_width, 0)
        product = jnp.dot(token_rows, weight_rows, preferred_element_type=jnp.float32)
        rounded = lax.optimization_barrier(product.astype(jnp.bfloat16))
        return running + rounded.astype(jnp.float32), None

    initial = jnp.zeros((tokens.shape[0], 2 * hidden_width), jnp.float32)
    summed, _ = lax.scan(accumulate, initial, jnp.arange(N_COL, dtype=jnp.int32))
    pre_gate = summed[:, :hidden_width]
    pre_up = summed[:, hidden_width:]
    hidden = (jax.nn.gelu(pre_gate, approximate=True) * pre_up).astype(jnp.bfloat16)
    return jnp.dot(hidden, w_down, preferred_element_type=jnp.float32).astype(jnp.bfloat16)
```

```python
import functools

import jax
import jax.numpy as jnp
from jax import lax
from jax.experimental import pallas as pl
from jax.experimental.pallas import tpu as pltpu
from jax.sharding import PartitionSpec as P

MESH = pl.DeviceIdType.MESH
PIECE = 16
TILE = 256


def activate(pre_gate, pre_up):
    return (jax.nn.gelu(pre_gate, approximate=True) * pre_up).astype(jnp.bfloat16)


def plain(tokens, w_gate, w_up, w_down):
    joined = jnp.concatenate([w_gate, w_up], axis=1)
    hidden_width = w_gate.shape[1]
    summed = lax.psum_scatter(
        jnp.dot(tokens, joined, preferred_element_type=jnp.float32).astype(jnp.bfloat16),
        "col",
        scatter_dimension=0,
        tiled=True,
    ).astype(jnp.float32)
    hidden = activate(summed[:, :hidden_width], summed[:, hidden_width:])
    hidden_all = lax.all_gather(hidden, "col", axis=0, tiled=True)
    result = lax.psum_scatter(
        jnp.dot(hidden_all, w_down, preferred_element_type=jnp.float32),
        "row",
        scatter_dimension=0,
        tiled=True,
    )
    return result.astype(jnp.bfloat16)


def kernel(
    n_row, chunks, tok_hbm, wg_hbm, wu_hbm, wd_hbm, out_ref,
    tok, w1, wd, s1, own, r1, s2, r2, hid, part, part16, c1r, c2s, c2r,
    load_sem, send1, recv1, send2, recv2, send3, recv3, send4, recv4, send5, recv5, send6, recv6,
):
    row, col = lax.axis_index("row"), lax.axis_index("col")
    y, x = col // 2, col % 2
    z, core = row // 2, row % 2
    n_z = n_row // 2
    half = w1.shape[2] // 2
    x_peer = (row, 2 * y + 1 - x)
    y_peer = (row, 2 * (1 - y) + x)
    core_peer = (2 * z + 1 - core, col)
    z_peers = [(2 * ((z + d) % n_z) + core, col) for d in range(1, n_z)]
    first_peer, second_peer = (x_peer, y_peer), (y_peer, x_peer)
    first_at, second_at = (x, y), (y, x)

    loads = [pltpu.make_async_copy(tok_hbm, tok, load_sem.at[0])]
    for mode in range(2):
        for k, w_hbm in enumerate((wg_hbm, wu_hbm)):
            loads.append(pltpu.make_async_copy(
                w_hbm.at[:, pl.ds(mode * half, half)],
                w1.at[mode, :, pl.ds(k * half, half)],
                load_sem.at[1 + 2 * mode + k],
            ))
    loads.append(pltpu.make_async_copy(wd_hbm, wd, load_sem.at[5]))
    for load in loads:
        load.start()

    barrier = pltpu.get_barrier_semaphore()
    peers = [x_peer, y_peer, core_peer] + z_peers
    for peer in peers:
        pl.semaphore_signal(barrier, inc=1, device_id=peer, device_id_type=MESH)

    def remote(src, dst, send_sem, recv_sem, peer):
        return pltpu.make_async_remote_copy(
            src_ref=src, dst_ref=dst, send_sem=send_sem, recv_sem=recv_sem, device_id=peer, device_id_type=MESH)

    def copy_s1(m, i):
        return remote(s1.at[m, i], r1.at[m, i], send1.at[m, i], recv1.at[m, i], first_peer[m])

    def copy_s2(m, i):
        return remote(s2.at[m, i], r2.at[m, i], send2.at[m, i], recv2.at[m, i], second_peer[m])

    def copy_g1(m, i):
        ref = hid.at[m, i, first_at[m], second_at[m]]
        return remote(ref, ref, send3.at[m, i], recv3.at[m, i], second_peer[m])

    def copy_g2(m, i):
        ref = hid.at[m, i, first_at[m]]
        return remote(ref, ref, send4.at[m, i], recv4.at[m, i], first_peer[m])

    def copy_c1(i):
        return remote(part16.at[i, 1 - core], c1r.at[i], send5.at[i], recv5.at[i], core_peer)

    def copy_c2(i, d):
        return remote(c2s.at[i, (z + d) % n_z], c2r.at[i, d - 1], send6.at[i, d - 1], recv6.at[i, d - 1], z_peers[d - 1])

    def product(m, mine, dst):
        at = first_at[m] if mine else 1 - first_at[m]
        rows = tok[:, at] if m == 0 else tok[at]
        rows = rows.reshape(-1, rows.shape[-1])

        @pl.loop(0, w1.shape[2] // TILE)
        def _(t):
            columns = pl.ds(pl.multiple_of(t * TILE, TILE), TILE)
            out = jnp.dot(rows, w1[m, :, columns], preferred_element_type=jnp.float32).astype(jnp.bfloat16)
            out = out.reshape(2, n_row // 4, chunks, PIECE, TILE)
            for i in range(chunks):
                dst[m, i, :, :, :, columns] = out[:, :, i]

    def f32(v):
        return v.astype(jnp.float32)

    def do_s1(i):
        for m in range(2):
            copy_s1(m, i).start()

    def do_s2(i):
        for m in range(2):
            copy_s1(m, i).wait_recv()
            at = 1 - second_at[m]
            s2[m, i] = (f32(own[m, i, at]) + f32(r1[m, i, at])).astype(jnp.bfloat16)
            copy_s2(m, i).start()

    def do_g1(i):
        for m in range(2):
            copy_s2(m, i).wait_recv()
            at = second_at[m]
            pre = f32(own[m, i, at]) + f32(r1[m, i, at]) + f32(r2[m, i])
            hid[m, i, first_at[m], at] = activate(pre[..., :half], pre[..., half:])
            copy_g1(m, i).start()

    def do_g2(i):
        for m in range(2):
            copy_g1(m, i).wait_recv()
            copy_g2(m, i).start()

    def do_c1(i):
        for m in range(2):
            copy_g2(m, i).wait_recv()
        rows = n_row // 4 * PIECE
        quarters = [
            jnp.concatenate([hid[0, i, b, a].reshape(rows, half), hid[1, i, a, b].reshape(rows, half)], axis=1)
            for a in range(2) for b in range(2)
        ]
        hidden = jnp.concatenate(quarters, axis=0)
        for t in range(wd.shape[1] // TILE):
            columns = slice(t * TILE, (t + 1) * TILE)
            out = jnp.dot(hidden, wd[:, columns], preferred_element_type=jnp.float32)
            out = out.reshape(n_z, 2, PIECE, TILE)
            for c in range(2):
                part[i, c, :, :, columns] = out[:, c]
                part16[i, c, :, :, columns] = out[:, c].astype(jnp.bfloat16)
        copy_c1(i).start()

    def do_c2(i):
        copy_c1(i).wait_recv()
        c2s[i] = (part[i, core] + f32(c1r[i])).astype(jnp.bfloat16)
        for d in range(1, n_z):
            copy_c2(i, d).start()

    def do_out(i):
        total = part[i, core, z] + f32(c1r[i, z])
        for d in range(1, n_z):
            copy_c2(i, d).wait_recv()
            total = total + f32(c2r[i, d - 1])
        out_ref[pl.ds(i * PIECE, PIECE), :] = total.astype(jnp.bfloat16)

    for load in loads[:3]:
        load.wait()
    product(0, False, s1)
    pl.semaphore_wait(barrier, len(peers))
    ahead = min(2, chunks)
    for i in range(ahead):
        copy_s1(0, i).start()
    for load in loads[3:5]:
        load.wait()
    product(1, False, s1)
    for i in range(ahead):
        copy_s1(1, i).start()
    product(0, True, own)
    product(1, True, own)
    loads[5].wait()

    for k in range(chunks + 6):
        for stage, late in ((do_s2, 0), (do_g1, 1), (do_s1, -2), (do_g2, 2), (do_c2, 4), (do_c1, 3), (do_out, 6)):
            i = k - late
            if 0 <= i < chunks and (stage is not do_s1 or i >= ahead):
                stage(i)

    for i in range(chunks):
        for m in range(2):
            for copy in (copy_s1, copy_s2, copy_g1, copy_g2):
                copy(m, i).wait_send()
        copy_c1(i).wait_send()
        for d in range(1, n_z):
            copy_c2(i, d).wait_send()


def fused(n_row, tokens, w_gate, w_up, w_down):
    n_tok, depth = tokens.shape
    width, features = w_down.shape
    per_row = n_tok // n_row
    chunks = per_row // PIECE
    n_z, blocks, half = n_row // 2, n_row // 4, width // 2
    bf16, dma = jnp.bfloat16, pltpu.SemaphoreType.DMA
    pair = [dma((2, chunks))] * 8
    return pl.pallas_call(
        functools.partial(kernel, n_row, chunks),
        out_shape=jax.ShapeDtypeStruct((per_row, features), bf16),
        in_specs=[pl.BlockSpec(memory_space=pl.ANY)] * 4,
        out_specs=pl.BlockSpec(memory_space=pltpu.VMEM),
        scratch_shapes=[
            pltpu.VMEM((2, 2, n_tok // 4, depth), bf16),
            pltpu.VMEM((2, depth, width), bf16),
            pltpu.VMEM((width, features), bf16),
            pltpu.VMEM((2, chunks, 2, blocks, PIECE, width), bf16),
            pltpu.VMEM((2, chunks, 2, blocks, PIECE, width), bf16),
            pltpu.VMEM((2, chunks, 2, blocks, PIECE, width), bf16),
            pltpu.VMEM((2, chunks, blocks, PIECE, width), bf16),
            pltpu.VMEM((2, chunks, blocks, PIECE, width), bf16),
            pltpu.VMEM((2, chunks, 2, 2, blocks, PIECE, half), bf16),
            pltpu.VMEM((chunks, 2, n_z, PIECE, features), jnp.float32),
            pltpu.VMEM((chunks, 2, n_z, PIECE, features), bf16),
            pltpu.VMEM((chunks, n_z, PIECE, features), bf16),
            pltpu.VMEM((chunks, n_z, PIECE, features), bf16),
            pltpu.VMEM((chunks, n_z - 1, PIECE, features), bf16),
            dma((6,)),
            *pair,
            dma((chunks,)), dma((chunks,)),
            dma((chunks, n_z - 1)), dma((chunks, n_z - 1)),
        ],
        compiler_params=pltpu.CompilerParams(
            collective_id=0, has_side_effects=True, vmem_limit_bytes=48 * 1024 * 1024
        ),
    )(tokens.reshape(2, 2, n_tok // 4, depth), w_gate, w_up, w_down)


def solution(mesh):
    n_row, n_col = mesh.shape["row"], mesh.shape["col"]

    def local(tokens, w_gate, w_up, w_down):
        width, features = w_down.shape
        fits = (
            n_col == 4
            and n_row % 4 == 0
            and n_row <= 16
            and tokens.shape[0] % (n_row * PIECE) == 0
            and tokens.shape[0] // (n_row * PIECE) <= 8
            and width % TILE == 0
            and features % TILE == 0
            and tokens.shape[1] * width <= 2 ** 21
            and width * features <= 2 ** 21
        )
        if fits:
            return fused(n_row, tokens, w_gate, w_up, w_down)
        return plain(tokens, w_gate, w_up, w_down)

    in_specs = (P(None, "col"), P("col", "row"), P("col", "row"), P("row", "col"))
    return jax.shard_map(local, mesh=mesh, in_specs=in_specs, out_specs=P("row", "col"), check_vma=False)
```

```python
import functools

import jax
import jax.numpy as jnp
from jax import lax
from jax.experimental import pallas as pl
from jax.experimental.pallas import tpu as pltpu
from jax.sharding import PartitionSpec as P

MESH = pl.DeviceIdType.MESH
PIECE = 16
TILE = 256


def activate(pre_gate, pre_up):
    return (jax.nn.gelu(pre_gate, approximate=True) * pre_up).astype(jnp.bfloat16)


def plain(tokens, w_gate, w_up, w_down):
    joined = jnp.concatenate([w_gate, w_up], axis=1)
    hidden_width = w_gate.shape[1]
    summed = lax.psum_scatter(
        jnp.dot(tokens, joined, preferred_element_type=jnp.float32).astype(jnp.bfloat16),
        "col",
        scatter_dimension=0,
        tiled=True,
    ).astype(jnp.float32)
    hidden = activate(summed[:, :hidden_width], summed[:, hidden_width:])
    hidden_all = lax.all_gather(hidden, "col", axis=0, tiled=True)
    result = lax.psum_scatter(
        jnp.dot(hidden_all, w_down, preferred_element_type=jnp.float32),
        "row",
        scatter_dimension=0,
        tiled=True,
    )
    return result.astype(jnp.bfloat16)


def kernel(
    n_row, chunks, tok_hbm, wg_hbm, wu_hbm, wd_hbm, out_ref,
    tok, w1, wd, s1, own, r1, s2, r2, hid, part, part16, c1r, c2s, c2r,
    load_sem, send1, recv1, send2, recv2, send3, recv3, send4, recv4, send5, recv5, send6, recv6,
):
    row, col = lax.axis_index("row"), lax.axis_index("col")
    y, x = col // 2, col % 2
    z, core = row // 2, row % 2
    n_z = n_row // 2
    half = w1.shape[2] // 2
    x_peer = (row, 2 * y + 1 - x)
    y_peer = (row, 2 * (1 - y) + x)
    core_peer = (2 * z + 1 - core, col)
    z_peers = [(2 * ((z + d) % n_z) + core, col) for d in range(1, n_z)]
    first_peer, second_peer = (x_peer, y_peer), (y_peer, x_peer)
    first_at, second_at = (x, y), (y, x)

    loads = [pltpu.make_async_copy(tok_hbm, tok, load_sem.at[0])]
    for mode in range(2):
        for k, w_hbm in enumerate((wg_hbm, wu_hbm)):
            loads.append(pltpu.make_async_copy(
                w_hbm.at[:, pl.ds(mode * half, half)],
                w1.at[mode, :, pl.ds(k * half, half)],
                load_sem.at[1 + 2 * mode + k],
            ))
    loads.append(pltpu.make_async_copy(wd_hbm, wd, load_sem.at[5]))
    for load in loads:
        load.start()

    barrier = pltpu.get_barrier_semaphore()
    peers = [x_peer, y_peer, core_peer] + z_peers
    for peer in peers:
        pl.semaphore_signal(barrier, inc=1, device_id=peer, device_id_type=MESH)

    def remote(src, dst, send_sem, recv_sem, peer):
        return pltpu.make_async_remote_copy(
            src_ref=src, dst_ref=dst, send_sem=send_sem, recv_sem=recv_sem, device_id=peer, device_id_type=MESH)

    def copy_s1(m, i):
        return remote(s1.at[m, i], r1.at[m, i], send1.at[m, i], recv1.at[m, i], first_peer[m])

    def copy_s2(m, i):
        return remote(s2.at[m, i], r2.at[m, i], send2.at[m, i], recv2.at[m, i], second_peer[m])

    def copy_g1(m, i):
        ref = hid.at[m, i, first_at[m], second_at[m]]
        return remote(ref, ref, send3.at[m, i], recv3.at[m, i], second_peer[m])

    def copy_g2(m, i):
        ref = hid.at[m, i, first_at[m]]
        return remote(ref, ref, send4.at[m, i], recv4.at[m, i], first_peer[m])

    def copy_c1(i):
        return remote(part16.at[i, 1 - core], c1r.at[i], send5.at[i], recv5.at[i], core_peer)

    def copy_c2(i, d):
        return remote(c2s.at[i, (z + d) % n_z], c2r.at[i, d - 1], send6.at[i, d - 1], recv6.at[i, d - 1], z_peers[d - 1])

    def product(m, mine, dst):
        at = first_at[m] if mine else 1 - first_at[m]
        rows = tok[:, at] if m == 0 else tok[at]
        rows = rows.reshape(-1, rows.shape[-1])

        @pl.loop(0, w1.shape[2] // TILE)
        def _(t):
            columns = pl.ds(pl.multiple_of(t * TILE, TILE), TILE)
            out = jnp.dot(rows, w1[m, :, columns], preferred_element_type=jnp.float32).astype(jnp.bfloat16)
            out = out.reshape(2, n_row // 4, chunks, PIECE, TILE)
            for i in range(chunks):
                dst[m, i, :, :, :, columns] = out[:, :, i]

    def f32(v):
        return v.astype(jnp.float32)

    def do_s1(i):
        for m in range(2):
            copy_s1(m, i).start()

    def do_s2(i):
        for m in range(2):
            copy_s1(m, i).wait_recv()
            at = 1 - second_at[m]
            s2[m, i] = (f32(own[m, i, at]) + f32(r1[m, i, at])).astype(jnp.bfloat16)
            copy_s2(m, i).start()

    def do_g1(i):
        for m in range(2):
            copy_s2(m, i).wait_recv()
            at = second_at[m]
            pre = f32(own[m, i, at]) + f32(r1[m, i, at]) + f32(r2[m, i])
            hid[m, i, first_at[m], at] = activate(pre[..., :half], pre[..., half:])
            copy_g1(m, i).start()

    def do_g2(i):
        for m in range(2):
            copy_g1(m, i).wait_recv()
            copy_g2(m, i).start()

    def do_c1(i):
        for m in range(2):
            copy_g2(m, i).wait_recv()
        rows = n_row // 4 * PIECE
        quarters = [
            jnp.concatenate([hid[0, i, b, a].reshape(rows, half), hid[1, i, a, b].reshape(rows, half)], axis=1)
            for a in range(2) for b in range(2)
        ]
        hidden = jnp.concatenate(quarters, axis=0)
        for t in range(wd.shape[1] // TILE):
            columns = slice(t * TILE, (t + 1) * TILE)
            out = jnp.dot(hidden, wd[:, columns], preferred_element_type=jnp.float32)
            out = out.reshape(n_z, 2, PIECE, TILE)
            for c in range(2):
                part[i, c, :, :, columns] = out[:, c]
                part16[i, c, :, :, columns] = out[:, c].astype(jnp.bfloat16)
        copy_c1(i).start()

    def do_c2(i):
        copy_c1(i).wait_recv()
        c2s[i] = (part[i, core] + f32(c1r[i])).astype(jnp.bfloat16)
        for d in range(1, n_z):
            copy_c2(i, d).start()

    def do_out(i):
        total = part[i, core, z] + f32(c1r[i, z])
        for d in range(1, n_z):
            copy_c2(i, d).wait_recv()
            total = total + f32(c2r[i, d - 1])
        out_ref[pl.ds(i * PIECE, PIECE), :] = total.astype(jnp.bfloat16)

    for load in loads[:3]:
        load.wait()
    product(0, False, s1)
    pl.semaphore_wait(barrier, len(peers))
    ahead = min(2, chunks)
    for i in range(ahead):
        copy_s1(0, i).start()
    for load in loads[3:5]:
        load.wait()
    product(1, False, s1)
    for i in range(ahead):
        copy_s1(1, i).start()
    product(0, True, own)
    product(1, True, own)
    loads[5].wait()

    for k in range(chunks + 6):
        for stage, late in ((do_s2, 0), (do_g1, 1), (do_s1, -2), (do_g2, 2), (do_c2, 4), (do_c1, 3), (do_out, 6)):
            i = k - late
            if 0 <= i < chunks and (stage is not do_s1 or i >= ahead):
                stage(i)

    for i in range(chunks):
        for m in range(2):
            for copy in (copy_s1, copy_s2, copy_g1, copy_g2):
                copy(m, i).wait_send()
        copy_c1(i).wait_send()
        for d in range(1, n_z):
            copy_c2(i, d).wait_send()


def fused(n_row, tokens, w_gate, w_up, w_down):
    n_tok, depth = tokens.shape
    width, features = w_down.shape
    per_row = n_tok // n_row
    chunks = per_row // PIECE
    n_z, blocks, half = n_row // 2, n_row // 4, width // 2
    bf16, dma = jnp.bfloat16, pltpu.SemaphoreType.DMA
    pair = [dma((2, chunks))] * 8
    return pl.pallas_call(
        functools.partial(kernel, n_row, chunks),
        out_shape=jax.ShapeDtypeStruct((per_row, features), bf16),
        in_specs=[pl.BlockSpec(memory_space=pl.ANY)] * 4,
        out_specs=pl.BlockSpec(memory_space=pltpu.VMEM),
        scratch_shapes=[
            pltpu.VMEM((2, 2, n_tok // 4, depth), bf16),
            pltpu.VMEM((2, depth, width), bf16),
            pltpu.VMEM((width, features), bf16),
            pltpu.VMEM((2, chunks, 2, blocks, PIECE, width), bf16),
            pltpu.VMEM((2, chunks, 2, blocks, PIECE, width), bf16),
            pltpu.VMEM((2, chunks, 2, blocks, PIECE, width), bf16),
            pltpu.VMEM((2, chunks, blocks, PIECE, width), bf16),
            pltpu.VMEM((2, chunks, blocks, PIECE, width), bf16),
            pltpu.VMEM((2, chunks, 2, 2, blocks, PIECE, half), bf16),
            pltpu.VMEM((chunks, 2, n_z, PIECE, features), jnp.float32),
            pltpu.VMEM((chunks, 2, n_z, PIECE, features), bf16),
            pltpu.VMEM((chunks, n_z, PIECE, features), bf16),
            pltpu.VMEM((chunks, n_z, PIECE, features), bf16),
            pltpu.VMEM((chunks, n_z - 1, PIECE, features), bf16),
            dma((6,)),
            *pair,
            dma((chunks,)), dma((chunks,)),
            dma((chunks, n_z - 1)), dma((chunks, n_z - 1)),
        ],
        compiler_params=pltpu.CompilerParams(
            collective_id=0, has_side_effects=True, vmem_limit_bytes=67043328
        ),
    )(tokens.reshape(2, 2, n_tok // 4, depth), w_gate, w_up, w_down)


def solution(mesh):
    n_row, n_col = mesh.shape["row"], mesh.shape["col"]

    def local(tokens, w_gate, w_up, w_down):
        width, features = w_down.shape
        fits = (
            n_col == 4
            and n_row % 4 == 0
            and n_row <= 16
            and tokens.shape[0] % (n_row * PIECE) == 0
            and tokens.shape[0] // (n_row * PIECE) <= 8
            and width % TILE == 0
            and features % TILE == 0
            and tokens.shape[1] * width <= 2 ** 21
            and width * features <= 2 ** 21
        )
        if fits:
            return fused(n_row, tokens, w_gate, w_up, w_down)
        return plain(tokens, w_gate, w_up, w_down)

    in_specs = (P(None, "col"), P("col", "row"), P("col", "row"), P("row", "col"))
    return jax.shard_map(local, mesh=mesh, in_specs=in_specs, out_specs=P("row", "col"), check_vma=False)
```

```python
import functools

import jax
import jax.numpy as jnp
from jax import lax
from jax.experimental import pallas as pl
from jax.experimental.pallas import tpu as pltpu
from jax.sharding import PartitionSpec as P

MESH = pl.DeviceIdType.MESH
PIECE = 8
TILE = 256


def activate(pre_gate, pre_up):
    return (jax.nn.gelu(pre_gate, approximate=True) * pre_up).astype(jnp.bfloat16)


def plain(tokens, w_gate, w_up, w_down):
    joined = jnp.concatenate([w_gate, w_up], axis=1)
    hidden_width = w_gate.shape[1]
    summed = lax.psum_scatter(
        jnp.dot(tokens, joined, preferred_element_type=jnp.float32).astype(jnp.bfloat16),
        "col",
        scatter_dimension=0,
        tiled=True,
    ).astype(jnp.float32)
    hidden = activate(summed[:, :hidden_width], summed[:, hidden_width:])
    hidden_all = lax.all_gather(hidden, "col", axis=0, tiled=True)
    result = lax.psum_scatter(
        jnp.dot(hidden_all, w_down, preferred_element_type=jnp.float32),
        "row",
        scatter_dimension=0,
        tiled=True,
    )
    return result.astype(jnp.bfloat16)


def kernel(
    n_row, chunks, tok_hbm, wg_hbm, wu_hbm, wd_hbm, out_hbm,
    tok, w1, wd, s1, own, r1, s2, r2, hid, part, part16, c1r, c2s, c2r, out_ref,
    load_sem, send1, recv1, send2, recv2, send3, recv3, send4, recv4, send5, recv5, send6, recv6, store_sem,
):
    row, col = lax.axis_index("row"), lax.axis_index("col")
    y, x = col // 2, col % 2
    z, core = row // 2, row % 2
    n_z = n_row // 2
    half = w1.shape[2] // 2
    x_peer = (row, 2 * y + 1 - x)
    y_peer = (row, 2 * (1 - y) + x)
    core_peer = (2 * z + 1 - core, col)
    upper = 2 * z // n_z

    def z_order(k):
        down = n_z - 1 - k - (z + k + 1) // n_z
        up = k + (k + n_z - z) // n_z
        return down * (1 - upper) + up * upper

    z_others = [z_order(k) for k in range(n_z - 1)]
    z_peers = [(2 * other + core, col) for other in z_others]
    first_peer, second_peer = (x_peer, y_peer), (y_peer, x_peer)
    first_at, second_at = (x, y), (y, x)

    loads = [pltpu.make_async_copy(tok_hbm, tok, load_sem.at[0])]
    for mode in range(2):
        for k, w_hbm in enumerate((wg_hbm, wu_hbm)):
            loads.append(pltpu.make_async_copy(
                w_hbm.at[:, pl.ds(mode * half, half)],
                w1.at[mode, :, pl.ds(k * half, half)],
                load_sem.at[1 + 2 * mode + k],
            ))
    loads.append(pltpu.make_async_copy(wd_hbm, wd, load_sem.at[5]))
    for load in loads:
        load.start()

    barrier = pltpu.get_barrier_semaphore()
    peers = [x_peer, y_peer, core_peer] + z_peers
    for peer in peers:
        pl.semaphore_signal(barrier, inc=1, device_id=peer, device_id_type=MESH)

    def remote(src, dst, send_sem, recv_sem, peer):
        return pltpu.make_async_remote_copy(
            src_ref=src, dst_ref=dst, send_sem=send_sem, recv_sem=recv_sem, device_id=peer, device_id_type=MESH)

    def copy_s1(m, i):
        return remote(s1.at[m, i], r1.at[m, i], send1.at[m, i], recv1.at[m, i], first_peer[m])

    def copy_s2(m, i):
        return remote(s2.at[m, i], r2.at[m, i], send2.at[m, i], recv2.at[m, i], second_peer[m])

    def copy_g1(m, i):
        ref = hid.at[m, i, first_at[m], second_at[m]]
        return remote(ref, ref, send3.at[m, i], recv3.at[m, i], second_peer[m])

    def copy_g2(m, i):
        ref = hid.at[m, i, first_at[m]]
        return remote(ref, ref, send4.at[m, i], recv4.at[m, i], first_peer[m])

    def copy_c1(i):
        return remote(part16.at[i, 1 - core], c1r.at[i], send5.at[i], recv5.at[i], core_peer)

    def copy_c2(i, k, arriving=False):
        at = z_others[k] if arriving else z
        return remote(c2s.at[i, z_others[k]], c2r.at[i, at], send6.at[i, k], recv6.at[i, at], z_peers[k])

    def store(i):
        rows = pl.ds(i * PIECE, PIECE)
        return pltpu.make_async_copy(out_ref.at[rows], out_hbm.at[rows], store_sem.at[i])

    def product(m, mine, dst, low, high):
        at = first_at[m] if mine else 1 - first_at[m]
        rows = tok[:, at, :, low:high] if m == 0 else tok[at, :, :, low:high]
        rows = rows.reshape(-1, rows.shape[-1])

        @pl.loop(0, w1.shape[2] // TILE)
        def _(t):
            columns = pl.ds(pl.multiple_of(t * TILE, TILE), TILE)
            out = jnp.dot(rows, w1[m, :, columns], preferred_element_type=jnp.float32).astype(jnp.bfloat16)
            out = out.reshape(2, n_row // 4, high - low, PIECE, TILE)
            for i in range(low, high):
                dst[m, i, :, :, :, columns] = out[:, :, i - low]

    def f32(v):
        return v.astype(jnp.float32)

    def do_s1(i):
        for m in range(2):
            copy_s1(m, i).start()

    def do_s2(i):
        for m in range(2):
            copy_s1(m, i).wait_recv()
            at = 1 - second_at[m]
            s2[m, i] = (f32(own[m, i, at]) + f32(r1[m, i, at])).astype(jnp.bfloat16)
            copy_s2(m, i).start()

    def do_g1(i):
        for m in range(2):
            copy_s2(m, i).wait_recv()
            at = second_at[m]
            pre = f32(own[m, i, at]) + f32(r1[m, i, at]) + f32(r2[m, i])
            hid[m, i, first_at[m], at] = activate(pre[..., :half], pre[..., half:])
            copy_g1(m, i).start()

    def do_g2(i):
        for m in range(2):
            copy_g1(m, i).wait_recv()
            copy_g2(m, i).start()

    def do_c1(i):
        for m in range(2):
            copy_g2(m, i).wait_recv()
        rows = n_row // 4 * PIECE
        quarters = [
            jnp.concatenate([hid[0, i, b, a].reshape(rows, half), hid[1, i, a, b].reshape(rows, half)], axis=1)
            for a in range(2) for b in range(2)
        ]
        hidden = jnp.concatenate(quarters, axis=0)
        for t in range(wd.shape[1] // TILE):
            columns = slice(t * TILE, (t + 1) * TILE)
            out = jnp.dot(hidden, wd[:, columns], preferred_element_type=jnp.float32)
            out = out.reshape(n_z, 2, PIECE, TILE)
            for c in range(2):
                part[i, c, :, :, columns] = out[:, c]
                part16[i, c, :, :, columns] = out[:, c].astype(jnp.bfloat16)
        copy_c1(i).start()

    def do_c2(i):
        copy_c1(i).wait_recv()
        c2s[i] = (part[i, core] + f32(c1r[i])).astype(jnp.bfloat16)
        for k in range(n_z - 1):
            copy_c2(i, k).start()

    def do_out(i):
        total = part[i, core, z] + f32(c1r[i, z])
        for k in reversed(range(n_z - 1)):
            copy_c2(i, k, True).wait_recv()
            total = total + f32(c2r[i, z_others[k]])
        out_ref[pl.ds(i * PIECE, PIECE), :] = total.astype(jnp.bfloat16)
        store(i).start()

    first = max(chunks // 4, 1)
    ahead = min(4, chunks)
    for load in loads[:3]:
        load.wait()
    product(0, False, s1, 0, first)
    pl.semaphore_wait(barrier, len(peers))
    for i in range(first):
        copy_s1(0, i).start()
    for load in loads[3:5]:
        load.wait()
    product(1, False, s1, 0, first)
    for i in range(first):
        copy_s1(1, i).start()
    for m in range(2):
        if first < chunks:
            product(m, False, s1, first, chunks)
            for i in range(first, ahead):
                copy_s1(m, i).start()
    product(0, True, own, 0, chunks)
    product(1, True, own, 0, chunks)
    loads[5].wait()

    for k in range(chunks + 6):
        for stage, late in ((do_s2, 0), (do_g1, 1), (do_s1, -2), (do_g2, 2), (do_c2, 4), (do_c1, 3), (do_out, 6)):
            i = k - late
            if 0 <= i < chunks and (stage is not do_s1 or i >= ahead):
                stage(i)

    for i in range(chunks):
        for m in range(2):
            for copy in (copy_s1, copy_s2, copy_g1, copy_g2):
                copy(m, i).wait_send()
        copy_c1(i).wait_send()
        for k in range(n_z - 1):
            copy_c2(i, k).wait_send()
        store(i).wait()


def fused(n_row, tokens, w_gate, w_up, w_down):
    n_tok, depth = tokens.shape
    width, features = w_down.shape
    per_row = n_tok // n_row
    chunks = per_row // PIECE
    n_z, blocks, half = n_row // 2, n_row // 4, width // 2
    bf16, dma = jnp.bfloat16, pltpu.SemaphoreType.DMA
    pair = [dma((2, chunks))] * 8
    return pl.pallas_call(
        functools.partial(kernel, n_row, chunks),
        out_shape=jax.ShapeDtypeStruct((per_row, features), bf16),
        in_specs=[pl.BlockSpec(memory_space=pl.ANY)] * 4,
        out_specs=pl.BlockSpec(memory_space=pl.ANY),
        scratch_shapes=[
            pltpu.VMEM((2, 2, blocks, chunks, PIECE, depth), bf16),
            pltpu.VMEM((2, depth, width), bf16),
            pltpu.VMEM((width, features), bf16),
            pltpu.VMEM((2, chunks, 2, blocks, PIECE, width), bf16),
            pltpu.VMEM((2, chunks, 2, blocks, PIECE, width), bf16),
            pltpu.VMEM((2, chunks, 2, blocks, PIECE, width), bf16),
            pltpu.VMEM((2, chunks, blocks, PIECE, width), bf16),
            pltpu.VMEM((2, chunks, blocks, PIECE, width), bf16),
            pltpu.VMEM((2, chunks, 2, 2, blocks, PIECE, half), bf16),
            pltpu.VMEM((chunks, 2, n_z, PIECE, features), jnp.float32),
            pltpu.VMEM((chunks, 2, n_z, PIECE, features), bf16),
            pltpu.VMEM((chunks, n_z, PIECE, features), bf16),
            pltpu.VMEM((chunks, n_z, PIECE, features), bf16),
            pltpu.VMEM((chunks, n_z, PIECE, features), bf16),
            pltpu.VMEM((per_row, features), bf16),
            dma((6,)),
            *pair,
            dma((chunks,)), dma((chunks,)),
            dma((chunks, n_z - 1)), dma((chunks, n_z)), dma((chunks,)),
        ],
        compiler_params=pltpu.CompilerParams(
            collective_id=0, has_side_effects=True, vmem_limit_bytes=67043328
        ),
    )(tokens.reshape(2, 2, blocks, chunks, PIECE, depth), w_gate, w_up, w_down)


def solution(mesh):
    n_row, n_col = mesh.shape["row"], mesh.shape["col"]

    def local(tokens, w_gate, w_up, w_down):
        width, features = w_down.shape
        fits = (
            n_col == 4
            and n_row % 4 == 0
            and n_row <= 16
            and tokens.shape[0] % (n_row * PIECE) == 0
            and tokens.shape[0] // (n_row * PIECE) <= 16
            and width % TILE == 0
            and features % TILE == 0
            and tokens.shape[1] * width <= 2 ** 21
            and width * features <= 2 ** 21
        )
        if fits:
            return fused(n_row, tokens, w_gate, w_up, w_down)
        return plain(tokens, w_gate, w_up, w_down)

    in_specs = (P(None, "col"), P("col", "row"), P("col", "row"), P("row", "col"))
    return jax.shard_map(local, mesh=mesh, in_specs=in_specs, out_specs=P("row", "col"), check_vma=False)
```

```python
import functools

import jax
import jax.numpy as jnp
from jax import lax
from jax.experimental import pallas as pl
from jax.experimental.pallas import tpu as pltpu
from jax.sharding import PartitionSpec as P

MESH = pl.DeviceIdType.MESH
PIECE = 8
TILE = 256


def activate(pre_gate, pre_up):
    return (jax.nn.gelu(pre_gate, approximate=True) * pre_up).astype(jnp.bfloat16)


def plain(tokens, w_gate, w_up, w_down):
    joined = jnp.concatenate([w_gate, w_up], axis=1)
    hidden_width = w_gate.shape[1]
    summed = lax.psum_scatter(
        jnp.dot(tokens, joined, preferred_element_type=jnp.float32).astype(jnp.bfloat16),
        "col",
        scatter_dimension=0,
        tiled=True,
    ).astype(jnp.float32)
    hidden = activate(summed[:, :hidden_width], summed[:, hidden_width:])
    hidden_all = lax.all_gather(hidden, "col", axis=0, tiled=True)
    result = lax.psum_scatter(
        jnp.dot(hidden_all, w_down, preferred_element_type=jnp.float32),
        "row",
        scatter_dimension=0,
        tiled=True,
    )
    return result.astype(jnp.bfloat16)


def chunk_rows(per_row):
    units = per_row // PIECE
    base = max(units // 4, 1)
    sizes = [base] * (units // base)
    sizes[0] += units - sum(sizes)
    if len(sizes) > 1 and base > 1:
        sizes[0] += base // 2
        sizes[-1] -= base // 2
    return [size * PIECE for size in sizes]


def kernel(
    n_row, sizes, tok_hbm, wg_hbm, wu_hbm, wd_hbm, out_hbm,
    tok, w1, wd, s1, own, r1, s2, r2, hid, part, part16, c1r, c2s, c2r, out_ref,
    load_sem, send1, recv1, send2, recv2, send3, recv3, send4, recv4, send5, recv5, send6, recv6, store_sem,
):
    row, col = lax.axis_index("row"), lax.axis_index("col")
    y, x = col // 2, col % 2
    z, core = row // 2, row % 2
    n_z = n_row // 2
    chunks = len(sizes)
    spans = [pl.ds(sum(sizes[:i]), sizes[i]) for i in range(chunks)]
    half = w1.shape[2] // 2
    x_peer = (row, 2 * y + 1 - x)
    y_peer = (row, 2 * (1 - y) + x)
    core_peer = (2 * z + 1 - core, col)
    upper = 2 * z // n_z

    def z_order(k):
        down = n_z - 1 - k - (z + k + 1) // n_z
        up = k + (k + n_z - z) // n_z
        return down * (1 - upper) + up * upper

    z_others = [z_order(k) for k in range(n_z - 1)]
    z_peers = [(2 * other + core, col) for other in z_others]
    first_peer, second_peer = (x_peer, y_peer), (y_peer, x_peer)
    first_at, second_at = (x, y), (y, x)

    loads = [pltpu.make_async_copy(tok_hbm, tok, load_sem.at[0])]
    for mode in range(2):
        for k, w_hbm in enumerate((wg_hbm, wu_hbm)):
            loads.append(pltpu.make_async_copy(
                w_hbm.at[:, pl.ds(mode * half, half)],
                w1.at[mode, :, pl.ds(k * half, half)],
                load_sem.at[1 + 2 * mode + k],
            ))
    loads.append(pltpu.make_async_copy(wd_hbm, wd, load_sem.at[5]))
    for load in loads[:3]:
        load.start()

    barrier = pltpu.get_barrier_semaphore()
    peers = [x_peer, y_peer, core_peer] + z_peers
    for peer in peers:
        pl.semaphore_signal(barrier, inc=1, device_id=peer, device_id_type=MESH)

    def remote(src, dst, send_sem, recv_sem, peer):
        return pltpu.make_async_remote_copy(
            src_ref=src, dst_ref=dst, send_sem=send_sem, recv_sem=recv_sem, device_id=peer, device_id_type=MESH)

    def copy_s1(m, i):
        return remote(s1.at[m, :, :, spans[i]], r1.at[m, :, :, spans[i]], send1.at[m, i], recv1.at[m, i], first_peer[m])

    def copy_s2(m, i):
        return remote(s2.at[m, :, spans[i]], r2.at[m, :, spans[i]], send2.at[m, i], recv2.at[m, i], second_peer[m])

    def copy_g1(m, i):
        ref = hid.at[m, first_at[m], second_at[m], :, spans[i]]
        return remote(ref, ref, send3.at[m, i], recv3.at[m, i], second_peer[m])

    def copy_g2(m, i):
        ref = hid.at[m, first_at[m], :, :, spans[i]]
        return remote(ref, ref, send4.at[m, i], recv4.at[m, i], first_peer[m])

    def copy_c1(i):
        return remote(part16.at[1 - core, :, spans[i]], c1r.at[:, spans[i]], send5.at[i], recv5.at[i], core_peer)

    def copy_c2(i, k, arriving=False):
        at = z_others[k] if arriving else z
        return remote(c2s.at[z_others[k], spans[i]], c2r.at[at, spans[i]], send6.at[i, k], recv6.at[i, at], z_peers[k])

    def store(i):
        return pltpu.make_async_copy(out_ref.at[spans[i]], out_hbm.at[spans[i]], store_sem.at[i])

    def product(m, mine, dst):
        at = first_at[m] if mine else 1 - first_at[m]
        rows = tok[:, at] if m == 0 else tok[at]
        shape = rows.shape[:-1]
        rows = rows.reshape(-1, rows.shape[-1])
        for t in range(w1.shape[2] // TILE):
            columns = slice(t * TILE, (t + 1) * TILE)
            out = jnp.dot(rows, w1[m, :, columns], preferred_element_type=jnp.float32)
            dst[m, :, :, :, columns] = out.astype(jnp.bfloat16).reshape(*shape, TILE)

    def f32(v):
        return v.astype(jnp.float32)

    def do_s1(i):
        for m in range(2):
            copy_s1(m, i).start()

    def do_s2(i):
        for m in range(2):
            copy_s1(m, i).wait_recv()
            at, span = 1 - second_at[m], spans[i]
            s2[m, :, span] = (f32(own[m, at, :, span]) + f32(r1[m, at, :, span])).astype(jnp.bfloat16)
            copy_s2(m, i).start()

    def do_g1(i):
        for m in range(2):
            copy_s2(m, i).wait_recv()
            at, span = second_at[m], spans[i]
            pre = f32(own[m, at, :, span]) + f32(r1[m, at, :, span]) + f32(r2[m, :, span])
            hid[m, first_at[m], at, :, span] = activate(pre[..., :half], pre[..., half:])
            copy_g1(m, i).start()

    def do_g2(i):
        for m in range(2):
            copy_g1(m, i).wait_recv()
            copy_g2(m, i).start()

    def do_c1(i):
        for m in range(2):
            copy_g2(m, i).wait_recv()
        span = spans[i]
        rows = n_row // 4 * sizes[i]
        quarters = [
            jnp.concatenate([hid[0, b, a, :, span].reshape(rows, half), hid[1, a, b, :, span].reshape(rows, half)], axis=1)
            for a in range(2) for b in range(2)
        ]
        hidden = jnp.concatenate(quarters, axis=0)
        for t in range(wd.shape[1] // TILE):
            columns = slice(t * TILE, (t + 1) * TILE)
            out = jnp.dot(hidden, wd[:, columns], preferred_element_type=jnp.float32)
            out = out.reshape(n_z, 2, sizes[i], TILE)
            for c in range(2):
                part[c, :, span, columns] = out[:, c]
                part16[c, :, span, columns] = out[:, c].astype(jnp.bfloat16)
        copy_c1(i).start()

    def do_c2(i):
        copy_c1(i).wait_recv()
        span = spans[i]
        c2s[:, span] = (part[core, :, span] + f32(c1r[:, span])).astype(jnp.bfloat16)
        for k in range(n_z - 1):
            copy_c2(i, k).start()

    def do_out(i):
        span = spans[i]
        total = part[core, z, span] + f32(c1r[z, span])
        for k in reversed(range(n_z - 1)):
            copy_c2(i, k, True).wait_recv()
            total = total + f32(c2r[z_others[k], span])
        out_ref[span] = total.astype(jnp.bfloat16)
        store(i).start()

    ahead = min(2, chunks)
    loads[0].wait()
    for load in loads[3:]:
        load.start()
    for load in loads[1:3]:
        load.wait()
    product(0, False, s1)
    pl.semaphore_wait(barrier, len(peers))
    for i in range(ahead):
        copy_s1(0, i).start()
    for load in loads[3:5]:
        load.wait()
    product(1, False, s1)
    for i in range(ahead):
        copy_s1(1, i).start()
    product(0, True, own)
    product(1, True, own)
    loads[5].wait()

    for k in range(chunks + 6):
        for stage, late in ((do_s2, 0), (do_g1, 1), (do_s1, -2), (do_g2, 2), (do_c2, 4), (do_c1, 3), (do_out, 6)):
            i = k - late
            if 0 <= i < chunks and (stage is not do_s1 or i >= ahead):
                stage(i)

    for i in range(chunks):
        for m in range(2):
            for copy in (copy_s1, copy_s2, copy_g1, copy_g2):
                copy(m, i).wait_send()
        copy_c1(i).wait_send()
        for k in range(n_z - 1):
            copy_c2(i, k).wait_send()
        store(i).wait()


def fused(n_row, tokens, w_gate, w_up, w_down):
    n_tok, depth = tokens.shape
    width, features = w_down.shape
    per_row = n_tok // n_row
    sizes = chunk_rows(per_row)
    chunks = len(sizes)
    n_z, blocks, half = n_row // 2, n_row // 4, width // 2
    bf16, dma = jnp.bfloat16, pltpu.SemaphoreType.DMA
    pair = [dma((2, chunks))] * 8
    return pl.pallas_call(
        functools.partial(kernel, n_row, sizes),
        out_shape=jax.ShapeDtypeStruct((per_row, features), bf16),
        in_specs=[pl.BlockSpec(memory_space=pl.ANY)] * 4,
        out_specs=pl.BlockSpec(memory_space=pl.ANY),
        scratch_shapes=[
            pltpu.VMEM((2, 2, blocks, per_row, depth), bf16),
            pltpu.VMEM((2, depth, width), bf16),
            pltpu.VMEM((width, features), bf16),
            pltpu.VMEM((2, 2, blocks, per_row, width), bf16),
            pltpu.VMEM((2, 2, blocks, per_row, width), bf16),
            pltpu.VMEM((2, 2, blocks, per_row, width), bf16),
            pltpu.VMEM((2, blocks, per_row, width), bf16),
            pltpu.VMEM((2, blocks, per_row, width), bf16),
            pltpu.VMEM((2, 2, 2, blocks, per_row, half), bf16),
            pltpu.VMEM((2, n_z, per_row, features), jnp.float32),
            pltpu.VMEM((2, n_z, per_row, features), bf16),
            pltpu.VMEM((n_z, per_row, features), bf16),
            pltpu.VMEM((n_z, per_row, features), bf16),
            pltpu.VMEM((n_z, per_row, features), bf16),
            pltpu.VMEM((per_row, features), bf16),
            dma((6,)),
            *pair,
            dma((chunks,)), dma((chunks,)),
            dma((chunks, n_z - 1)), dma((chunks, n_z)), dma((chunks,)),
        ],
        compiler_params=pltpu.CompilerParams(
            collective_id=0, has_side_effects=True, vmem_limit_bytes=67043328
        ),
    )(tokens.reshape(2, 2, blocks, per_row, depth), w_gate, w_up, w_down)


def solution(mesh):
    n_row, n_col = mesh.shape["row"], mesh.shape["col"]

    def local(tokens, w_gate, w_up, w_down):
        width, features = w_down.shape
        fits = (
            n_col == 4
            and n_row % 4 == 0
            and n_row <= 16
            and tokens.shape[0] % (n_row * PIECE) == 0
            and tokens.shape[0] // (n_row * PIECE) <= 16
            and width % TILE == 0
            and features % TILE == 0
            and tokens.shape[1] * width <= 2 ** 21
            and width * features <= 2 ** 21
        )
        if fits:
            return fused(n_row, tokens, w_gate, w_up, w_down)
        return plain(tokens, w_gate, w_up, w_down)

    in_specs = (P(None, "col"), P("col", "row"), P("col", "row"), P("row", "col"))
    return jax.shard_map(local, mesh=mesh, in_specs=in_specs, out_specs=P("row", "col"), check_vma=False)
```

```python
import functools

import jax
import jax.numpy as jnp
from jax import lax
from jax.experimental import pallas as pl
from jax.experimental.pallas import tpu as pltpu
from jax.sharding import PartitionSpec as P

MESH = pl.DeviceIdType.MESH
PIECE = 8
TILE = 256


def activate(pre_gate, pre_up):
    return (jax.nn.gelu(pre_gate, approximate=True) * pre_up).astype(jnp.bfloat16)


def plain(tokens, w_gate, w_up, w_down):
    joined = jnp.concatenate([w_gate, w_up], axis=1)
    hidden_width = w_gate.shape[1]
    summed = lax.psum_scatter(
        jnp.dot(tokens, joined, preferred_element_type=jnp.float32).astype(jnp.bfloat16),
        "col",
        scatter_dimension=0,
        tiled=True,
    ).astype(jnp.float32)
    hidden = activate(summed[:, :hidden_width], summed[:, hidden_width:])
    hidden_all = lax.all_gather(hidden, "col", axis=0, tiled=True)
    result = lax.psum_scatter(
        jnp.dot(hidden_all, w_down, preferred_element_type=jnp.float32),
        "row",
        scatter_dimension=0,
        tiled=True,
    )
    return result.astype(jnp.bfloat16)


def chunk_rows(per_row):
    units = per_row // PIECE
    sizes = [1, 1, 2, 2, 1, 1] if units % 8 == 0 else [1] * units
    return [size * per_row // sum(sizes) for size in sizes]


def kernel(
    n_row, sizes, tok_hbm, wg_hbm, wu_hbm, wd_hbm, out_hbm,
    tok, w1, wd, s1, own, r1, s2, r2, hid, part, part16, c1r, c2s, c2r, out_ref,
    load_sem, send1, recv1, send2, recv2, send3, recv3, send4, recv4, send5, recv5, send6, recv6, store_sem,
):
    row, col = lax.axis_index("row"), lax.axis_index("col")
    y, x = col // 2, col % 2
    z, core = row // 2, row % 2
    n_z = n_row // 2
    chunks = len(sizes)
    spans = [pl.ds(sum(sizes[:i]), sizes[i]) for i in range(chunks)]
    half = w1.shape[2] // 2
    x_peer = (row, 2 * y + 1 - x)
    y_peer = (row, 2 * (1 - y) + x)
    core_peer = (2 * z + 1 - core, col)
    upper = 2 * z // n_z

    def z_order(k):
        down = n_z - 1 - k - (z + k + 1) // n_z
        up = k + (k + n_z - z) // n_z
        return down * (1 - upper) + up * upper

    z_others = [z_order(k) for k in range(n_z - 1)]
    z_peers = [(2 * other + core, col) for other in z_others]
    first_peer, second_peer = (x_peer, y_peer), (y_peer, x_peer)
    first_at, second_at = (x, y), (y, x)

    loads = [pltpu.make_async_copy(tok_hbm, tok, load_sem.at[0])]
    for mode in range(2):
        for k, w_hbm in enumerate((wg_hbm, wu_hbm)):
            loads.append(pltpu.make_async_copy(
                w_hbm.at[:, pl.ds(mode * half, half)],
                w1.at[mode, :, pl.ds(k * half, half)],
                load_sem.at[1 + 2 * mode + k],
            ))
    loads.append(pltpu.make_async_copy(wd_hbm, wd, load_sem.at[5]))
    for load in loads[:3]:
        load.start()

    barrier = pltpu.get_barrier_semaphore()
    peers = [x_peer, y_peer, core_peer] + z_peers
    for peer in peers:
        pl.semaphore_signal(barrier, inc=1, device_id=peer, device_id_type=MESH)

    def remote(src, dst, send_sem, recv_sem, peer):
        return pltpu.make_async_remote_copy(
            src_ref=src, dst_ref=dst, send_sem=send_sem, recv_sem=recv_sem, device_id=peer, device_id_type=MESH)

    def copy_s1(m, i):
        return remote(s1.at[m, :, :, spans[i]], r1.at[m, :, :, spans[i]], send1.at[m, i], recv1.at[m, i], first_peer[m])

    def copy_s2(m, i):
        return remote(s2.at[m, :, spans[i]], r2.at[m, :, spans[i]], send2.at[m, i], recv2.at[m, i], second_peer[m])

    def copy_g1(m, i):
        ref = hid.at[m, first_at[m], second_at[m], :, spans[i]]
        return remote(ref, ref, send3.at[m, i], recv3.at[m, i], second_peer[m])

    def copy_g2(m, i):
        ref = hid.at[m, first_at[m], :, :, spans[i]]
        return remote(ref, ref, send4.at[m, i], recv4.at[m, i], first_peer[m])

    def copy_c1(i):
        return remote(part16.at[1 - core, :, spans[i]], c1r.at[:, spans[i]], send5.at[i], recv5.at[i], core_peer)

    def copy_c2(i, k, arriving=False):
        at = z_others[k] if arriving else z
        return remote(c2s.at[z_others[k], spans[i]], c2r.at[at, spans[i]], send6.at[i, k], recv6.at[i, at], z_peers[k])

    def store(i):
        return pltpu.make_async_copy(out_ref.at[spans[i]], out_hbm.at[spans[i]], store_sem.at[i])

    def product(m, mine, dst, low, high):
        at = first_at[m] if mine else 1 - first_at[m]
        rows = tok[:, at, :, low:high] if m == 0 else tok[at, :, :, low:high]
        shape = rows.shape[:-1]
        rows = rows.reshape(-1, rows.shape[-1])
        for t in range(w1.shape[2] // TILE):
            columns = slice(t * TILE, (t + 1) * TILE)
            out = jnp.dot(rows, w1[m, :, columns], preferred_element_type=jnp.float32)
            dst[m, :, :, low:high, columns] = out.astype(jnp.bfloat16).reshape(*shape, TILE)

    def f32(v):
        return v.astype(jnp.float32)

    def do_s1(i):
        for m in range(2):
            copy_s1(m, i).start()

    def do_s2(i):
        for m in range(2):
            copy_s1(m, i).wait_recv()
            at, span = 1 - second_at[m], spans[i]
            s2[m, :, span] = (f32(own[m, at, :, span]) + f32(r1[m, at, :, span])).astype(jnp.bfloat16)
            copy_s2(m, i).start()

    def do_g1(i):
        for m in range(2):
            copy_s2(m, i).wait_recv()
            at, span = second_at[m], spans[i]
            pre = f32(own[m, at, :, span]) + f32(r1[m, at, :, span]) + f32(r2[m, :, span])
            hid[m, first_at[m], at, :, span] = activate(pre[..., :half], pre[..., half:])
            copy_g1(m, i).start()

    def do_g2(i):
        for m in range(2):
            copy_g1(m, i).wait_recv()
            copy_g2(m, i).start()

    def do_c1(i):
        for m in range(2):
            copy_g2(m, i).wait_recv()
        span = spans[i]
        rows = n_row // 4 * sizes[i]
        quarters = [
            jnp.concatenate([hid[0, b, a, :, span].reshape(rows, half), hid[1, a, b, :, span].reshape(rows, half)], axis=1)
            for a in range(2) for b in range(2)
        ]
        hidden = jnp.concatenate(quarters, axis=0)
        for t in range(wd.shape[1] // TILE):
            columns = slice(t * TILE, (t + 1) * TILE)
            out = jnp.dot(hidden, wd[:, columns], preferred_element_type=jnp.float32)
            out = out.reshape(n_z, 2, sizes[i], TILE)
            for c in range(2):
                part[c, :, span, columns] = out[:, c]
                part16[c, :, span, columns] = out[:, c].astype(jnp.bfloat16)
        copy_c1(i).start()

    def do_c2(i):
        copy_c1(i).wait_recv()
        span = spans[i]
        c2s[:, span] = (part[core, :, span] + f32(c1r[:, span])).astype(jnp.bfloat16)
        for k in range(n_z - 1):
            copy_c2(i, k).start()

    def do_out(i):
        span = spans[i]
        total = part[core, z, span] + f32(c1r[z, span])
        for k in reversed(range(n_z - 1)):
            copy_c2(i, k, True).wait_recv()
            total = total + f32(c2r[z_others[k], span])
        out_ref[span] = total.astype(jnp.bfloat16)
        store(i).start()

    first, ahead = min(2, chunks), min(3, chunks)
    cut, end = sum(sizes[:first]), sum(sizes)
    loads[0].wait()
    for load in loads[3:]:
        load.start()
    for m in range(2):
        for load in loads[1 + 2 * m:3 + 2 * m]:
            load.wait()
        product(m, False, s1, 0, cut)
        if m == 0:
            pl.semaphore_wait(barrier, len(peers))
        for i in range(first):
            copy_s1(m, i).start()
    for m in range(2):
        if cut < end:
            product(m, False, s1, cut, end)
            for i in range(first, ahead):
                copy_s1(m, i).start()
    for m in range(2):
        product(m, True, own, 0, end)
    loads[5].wait()

    for k in range(chunks + 4):
        for stage, late in ((do_s2, 0), (do_g1, 1), (do_s1, -2), (do_g2, 2), (do_c2, 4), (do_c1, 3)):
            i = k - late
            if 0 <= i < chunks and (stage is not do_s1 or i >= ahead):
                stage(i)
    for i in range(chunks):
        do_out(i)

    for i in range(chunks):
        for m in range(2):
            for copy in (copy_s1, copy_s2, copy_g1, copy_g2):
                copy(m, i).wait_send()
        copy_c1(i).wait_send()
        for k in range(n_z - 1):
            copy_c2(i, k).wait_send()
        store(i).wait()


def fused(n_row, tokens, w_gate, w_up, w_down):
    n_tok, depth = tokens.shape
    width, features = w_down.shape
    per_row = n_tok // n_row
    sizes = chunk_rows(per_row)
    chunks = len(sizes)
    n_z, blocks, half = n_row // 2, n_row // 4, width // 2
    bf16, dma = jnp.bfloat16, pltpu.SemaphoreType.DMA
    pair = [dma((2, chunks))] * 8
    return pl.pallas_call(
        functools.partial(kernel, n_row, sizes),
        out_shape=jax.ShapeDtypeStruct((per_row, features), bf16),
        in_specs=[pl.BlockSpec(memory_space=pl.ANY)] * 4,
        out_specs=pl.BlockSpec(memory_space=pl.ANY),
        scratch_shapes=[
            pltpu.VMEM((2, 2, blocks, per_row, depth), bf16),
            pltpu.VMEM((2, depth, width), bf16),
            pltpu.VMEM((width, features), bf16),
            pltpu.VMEM((2, 2, blocks, per_row, width), bf16),
            pltpu.VMEM((2, 2, blocks, per_row, width), bf16),
            pltpu.VMEM((2, 2, blocks, per_row, width), bf16),
            pltpu.VMEM((2, blocks, per_row, width), bf16),
            pltpu.VMEM((2, blocks, per_row, width), bf16),
            pltpu.VMEM((2, 2, 2, blocks, per_row, half), bf16),
            pltpu.VMEM((2, n_z, per_row, features), jnp.float32),
            pltpu.VMEM((2, n_z, per_row, features), bf16),
            pltpu.VMEM((n_z, per_row, features), bf16),
            pltpu.VMEM((n_z, per_row, features), bf16),
            pltpu.VMEM((n_z, per_row, features), bf16),
            pltpu.VMEM((per_row, features), bf16),
            dma((6,)),
            *pair,
            dma((chunks,)), dma((chunks,)),
            dma((chunks, n_z - 1)), dma((chunks, n_z)), dma((chunks,)),
        ],
        compiler_params=pltpu.CompilerParams(
            collective_id=0, has_side_effects=True, vmem_limit_bytes=67043328
        ),
    )(tokens.reshape(2, 2, blocks, per_row, depth), w_gate, w_up, w_down)


def solution(mesh):
    n_row, n_col = mesh.shape["row"], mesh.shape["col"]

    def local(tokens, w_gate, w_up, w_down):
        width, features = w_down.shape
        fits = (
            n_col == 4
            and n_row % 4 == 0
            and n_row <= 16
            and tokens.shape[0] % (n_row * PIECE) == 0
            and tokens.shape[0] // (n_row * PIECE) <= 16
            and width % TILE == 0
            and features % TILE == 0
            and tokens.shape[1] * width <= 2 ** 21
            and width * features <= 2 ** 21
        )
        if fits:
            return fused(n_row, tokens, w_gate, w_up, w_down)
        return plain(tokens, w_gate, w_up, w_down)

    in_specs = (P(None, "col"), P("col", "row"), P("col", "row"), P("row", "col"))
    return jax.shard_map(local, mesh=mesh, in_specs=in_specs, out_specs=P("row", "col"), check_vma=False)
```

```python
import functools

import jax
import jax.numpy as jnp
from jax import lax
from jax.experimental import pallas as pl
from jax.experimental.pallas import tpu as pltpu
from jax.sharding import PartitionSpec as P

MESH = pl.DeviceIdType.MESH
PIECE = 8
TILE = 256


def activate(pre_gate, pre_up):
    return (jax.nn.gelu(pre_gate, approximate=True) * pre_up).astype(jnp.bfloat16)


def plain(tokens, w_gate, w_up, w_down):
    joined = jnp.concatenate([w_gate, w_up], axis=1)
    hidden_width = w_gate.shape[1]
    summed = lax.psum_scatter(
        jnp.dot(tokens, joined, preferred_element_type=jnp.float32).astype(jnp.bfloat16),
        "col",
        scatter_dimension=0,
        tiled=True,
    ).astype(jnp.float32)
    hidden = activate(summed[:, :hidden_width], summed[:, hidden_width:])
    hidden_all = lax.all_gather(hidden, "col", axis=0, tiled=True)
    result = lax.psum_scatter(
        jnp.dot(hidden_all, w_down, preferred_element_type=jnp.float32),
        "row",
        scatter_dimension=0,
        tiled=True,
    )
    return result.astype(jnp.bfloat16)


def chunk_rows(per_row):
    units = per_row // PIECE
    sizes = [1, 1, 2, 2, 1, 1] if units % 8 == 0 else [1] * units
    return [size * per_row // sum(sizes) for size in sizes]


def kernel(
    n_row, sizes, tok_hbm, wg_hbm, wu_hbm, wd_hbm, out_hbm,
    tok, w1, wd, s1, own, r1, s2, r2, hid, part, part16, c1r, c2s, c2r, out_ref,
    load_sem, send1, recv1, send2, recv2, send3, recv3, send4, recv4, send5, recv5, send6, recv6, store_sem,
):
    row, col = lax.axis_index("row"), lax.axis_index("col")
    y, x = col // 2, col % 2
    z, core = row // 2, row % 2
    n_z = n_row // 2
    chunks = len(sizes)
    spans = [pl.ds(sum(sizes[:i]), sizes[i]) for i in range(chunks)]
    half = w1.shape[2] // 2
    x_peer = (row, 2 * y + 1 - x)
    y_peer = (row, 2 * (1 - y) + x)
    core_peer = (2 * z + 1 - core, col)
    upper = 2 * z // n_z

    def z_order(k):
        down = n_z - 1 - k - (z + k + 1) // n_z
        up = k + (k + n_z - z) // n_z
        return down * (1 - upper) + up * upper

    z_others = [z_order(k) for k in range(n_z - 1)]
    z_peers = [(2 * other + core, col) for other in z_others]
    first_peer, second_peer = (x_peer, y_peer), (y_peer, x_peer)
    first_at, second_at = (x, y), (y, x)

    loads = [pltpu.make_async_copy(tok_hbm, tok, load_sem.at[0])]
    for mode in range(2):
        for k, w_hbm in enumerate((wg_hbm, wu_hbm)):
            loads.append(pltpu.make_async_copy(
                w_hbm.at[:, pl.ds(mode * half, half)],
                w1.at[mode, :, pl.ds(k * half, half)],
                load_sem.at[1 + 2 * mode + k],
            ))
    loads.append(pltpu.make_async_copy(wd_hbm, wd, load_sem.at[5]))
    for load in loads[:3]:
        load.start()

    barrier = pltpu.get_barrier_semaphore()
    peers = [x_peer, y_peer, core_peer] + z_peers
    for peer in peers:
        pl.semaphore_signal(barrier, inc=1, device_id=peer, device_id_type=MESH)

    def remote(src, dst, send_sem, recv_sem, peer):
        return pltpu.make_async_remote_copy(
            src_ref=src, dst_ref=dst, send_sem=send_sem, recv_sem=recv_sem, device_id=peer, device_id_type=MESH)

    def copy_s1(m, i):
        return remote(s1.at[m, :, :, spans[i]], r1.at[m, :, :, spans[i]], send1.at[m, i], recv1.at[m, i], first_peer[m])

    def copy_s2(m, i):
        return remote(s2.at[m, :, spans[i]], r2.at[m, :, spans[i]], send2.at[m, i], recv2.at[m, i], second_peer[m])

    def copy_g1(m, i):
        ref = hid.at[m, first_at[m], second_at[m], :, spans[i]]
        return remote(ref, ref, send3.at[m, i], recv3.at[m, i], second_peer[m])

    def copy_g2(m, i):
        ref = hid.at[m, first_at[m], :, :, spans[i]]
        return remote(ref, ref, send4.at[m, i], recv4.at[m, i], first_peer[m])

    def copy_c1(i):
        return remote(part16.at[1 - core, :, spans[i]], c1r.at[:, spans[i]], send5.at[i], recv5.at[i], core_peer)

    def copy_c2(i, k, arriving=False):
        at = z_others[k] if arriving else z
        return remote(c2s.at[z_others[k], spans[i]], c2r.at[at, spans[i]], send6.at[i, k], recv6.at[i, at], z_peers[k])

    def store(i):
        return pltpu.make_async_copy(out_ref.at[spans[i]], out_hbm.at[spans[i]], store_sem.at[i])

    def product(m, mine, dst, low, high):
        at = first_at[m] if mine else 1 - first_at[m]
        rows = tok[:, at, :, low:high] if m == 0 else tok[at, :, :, low:high]
        shape = rows.shape[:-1]
        rows = rows.reshape(-1, rows.shape[-1])
        for t in range(w1.shape[2] // TILE):
            columns = slice(t * TILE, (t + 1) * TILE)
            out = jnp.dot(rows, w1[m, :, columns], preferred_element_type=jnp.float32)
            dst[m, :, :, low:high, columns] = out.astype(jnp.bfloat16).reshape(*shape, TILE)

    def f32(v):
        return v.astype(jnp.float32)

    def do_s1(i):
        for m in range(2):
            copy_s1(m, i).start()

    def do_s2(i):
        for m in range(2):
            copy_s1(m, i).wait_recv()
            at, span = 1 - second_at[m], spans[i]
            s2[m, :, span] = (f32(own[m, at, :, span]) + f32(r1[m, at, :, span])).astype(jnp.bfloat16)
            copy_s2(m, i).start()

    def do_g1(i):
        for m in range(2):
            copy_s2(m, i).wait_recv()
            at, span = second_at[m], spans[i]
            pre = f32(own[m, at, :, span]) + f32(r1[m, at, :, span]) + f32(r2[m, :, span])
            hid[m, first_at[m], at, :, span] = activate(pre[..., :half], pre[..., half:])
            copy_g1(m, i).start()

    def do_g2(i):
        for m in range(2):
            copy_g1(m, i).wait_recv()
            copy_g2(m, i).start()

    def do_c1(i):
        for m in range(2):
            copy_g2(m, i).wait_recv()
        span = spans[i]
        rows = n_row // 4 * sizes[i]
        quarters = [
            jnp.concatenate([hid[0, b, a, :, span].reshape(rows, half), hid[1, a, b, :, span].reshape(rows, half)], axis=1)
            for a in range(2) for b in range(2)
        ]
        hidden = jnp.concatenate(quarters, axis=0)
        for t in range(wd.shape[1] // TILE):
            columns = slice(t * TILE, (t + 1) * TILE)
            out = jnp.dot(hidden, wd[:, columns], preferred_element_type=jnp.float32)
            out = out.reshape(n_z, 2, sizes[i], TILE)
            for c in range(2):
                part[c, :, span, columns] = out[:, c]
                part16[c, :, span, columns] = out[:, c].astype(jnp.bfloat16)
        copy_c1(i).start()

    def do_c2(i):
        copy_c1(i).wait_recv()
        span = spans[i]
        c2s[:, span] = (part[core, :, span] + f32(c1r[:, span])).astype(jnp.bfloat16)
        for k in range(n_z - 1):
            copy_c2(i, k).start()

    def do_out(i):
        span = spans[i]
        total = part[core, z, span] + f32(c1r[z, span])
        for k in reversed(range(n_z - 1)):
            copy_c2(i, k, True).wait_recv()
            total = total + f32(c2r[z_others[k], span])
        out_ref[span] = total.astype(jnp.bfloat16)
        store(i).start()

    first, ahead = min(2, chunks), min(3, chunks)
    cut, end = sum(sizes[:first]), sum(sizes)
    loads[0].wait()
    for load in loads[3:]:
        load.start()
    for m in range(2):
        for load in loads[1 + 2 * m:3 + 2 * m]:
            load.wait()
        product(m, False, s1, 0, cut)
        if m == 0:
            pl.semaphore_wait(barrier, len(peers))
        for i in range(first):
            copy_s1(m, i).start()
    for m in range(2):
        if cut < end:
            product(m, False, s1, cut, end)
            for i in range(first, ahead):
                copy_s1(m, i).start()
    for m in range(2):
        product(m, True, own, 0, end)
    loads[5].wait()

    for k in range(chunks + 4):
        for stage, late in ((do_s2, 0), (do_g1, 1), (do_s1, -3), (do_g2, 2), (do_c2, 4), (do_c1, 3)):
            i = k - late
            if 0 <= i < chunks and (stage is not do_s1 or i >= ahead):
                stage(i)
    for i in range(chunks):
        do_out(i)

    for i in range(chunks):
        for m in range(2):
            for copy in (copy_s1, copy_s2, copy_g1, copy_g2):
                copy(m, i).wait_send()
        copy_c1(i).wait_send()
        for k in range(n_z - 1):
            copy_c2(i, k).wait_send()
        store(i).wait()


def fused(n_row, tokens, w_gate, w_up, w_down):
    n_tok, depth = tokens.shape
    width, features = w_down.shape
    per_row = n_tok // n_row
    sizes = chunk_rows(per_row)
    chunks = len(sizes)
    n_z, blocks, half = n_row // 2, n_row // 4, width // 2
    bf16, dma = jnp.bfloat16, pltpu.SemaphoreType.DMA
    pair = [dma((2, chunks))] * 8
    return pl.pallas_call(
        functools.partial(kernel, n_row, sizes),
        out_shape=jax.ShapeDtypeStruct((per_row, features), bf16),
        in_specs=[pl.BlockSpec(memory_space=pl.ANY)] * 4,
        out_specs=pl.BlockSpec(memory_space=pl.ANY),
        scratch_shapes=[
            pltpu.VMEM((2, 2, blocks, per_row, depth), bf16),
            pltpu.VMEM((2, depth, width), bf16),
            pltpu.VMEM((width, features), bf16),
            pltpu.VMEM((2, 2, blocks, per_row, width), bf16),
            pltpu.VMEM((2, 2, blocks, per_row, width), bf16),
            pltpu.VMEM((2, 2, blocks, per_row, width), bf16),
            pltpu.VMEM((2, blocks, per_row, width), bf16),
            pltpu.VMEM((2, blocks, per_row, width), bf16),
            pltpu.VMEM((2, 2, 2, blocks, per_row, half), bf16),
            pltpu.VMEM((2, n_z, per_row, features), jnp.float32),
            pltpu.VMEM((2, n_z, per_row, features), bf16),
            pltpu.VMEM((n_z, per_row, features), bf16),
            pltpu.VMEM((n_z, per_row, features), bf16),
            pltpu.VMEM((n_z, per_row, features), bf16),
            pltpu.VMEM((per_row, features), bf16),
            dma((6,)),
            *pair,
            dma((chunks,)), dma((chunks,)),
            dma((chunks, n_z - 1)), dma((chunks, n_z)), dma((chunks,)),
        ],
        compiler_params=pltpu.CompilerParams(
            collective_id=0, has_side_effects=True, vmem_limit_bytes=67043328
        ),
    )(tokens.reshape(2, 2, blocks, per_row, depth), w_gate, w_up, w_down)


def solution(mesh):
    n_row, n_col = mesh.shape["row"], mesh.shape["col"]

    def local(tokens, w_gate, w_up, w_down):
        width, features = w_down.shape
        fits = (
            n_col == 4
            and n_row % 4 == 0
            and n_row <= 16
            and tokens.shape[0] % (n_row * PIECE) == 0
            and tokens.shape[0] // (n_row * PIECE) <= 16
            and width % TILE == 0
            and features % TILE == 0
            and tokens.shape[1] * width <= 2 ** 21
            and width * features <= 2 ** 21
        )
        if fits:
            return fused(n_row, tokens, w_gate, w_up, w_down)
        return plain(tokens, w_gate, w_up, w_down)

    in_specs = (P(None, "col"), P("col", "row"), P("col", "row"), P("row", "col"))
    return jax.shard_map(local, mesh=mesh, in_specs=in_specs, out_specs=P("row", "col"), check_vma=False)
```
